32 devices in a mesh: dp: 4 (over x, core), head: 8 (over z, y).
Axes of the slice: x: 2, y: 2, z: 4, core: 2. Of those that a mesh axis runs over, the one named last changes fastest.
Arguments:
- tokens: bfloat16 [24576, 1152], P(('dp', 'head')), may hold values from -6 to 6
- segment_ids: int32 [24576], P('dp'), may hold values from 0 to 95, as said below
- cond: float32 [96, 1152], P('dp'), may hold values from -6 to 6
- w_ada: bfloat16 [1152, 6912], P(None, 'head'), may hold values from -0.1875 to 0.1875
- b_ada: bfloat16 [6912], P('head'), may hold values from -4 to 4
- w_qkv: bfloat16 [1152, 3, 1152], P(None, None, 'head'), may hold values from -0.1875 to 0.1875
- bias_qv: bfloat16 [2, 1152], P(None, 'head'), may hold values from -4 to 4
- w_proj: bfloat16 [1152, 1152], P('head'), may hold values from -0.75 to 0.75
- b_proj: bfloat16 [1152], replicated, may hold values from -4 to 4
- w_fc1: bfloat16 [1152, 4608], P(None, 'head'), may hold values from -0.1875 to 0.1875
- b_fc1: bfloat16 [4608], P('head'), may hold values from -4 to 4
- w_fc2: bfloat16 [4608, 1152], P('head'), may hold values from -0.09375 to 0.09375
- b_fc2: bfloat16 [1152], replicated, may hold values from -4 to 4
- cotangent: bfloat16 [24576, 1152], P(('dp', 'head')), may hold values from -6 to 6
Outputs:
- out: bfloat16 [24576, 1152], P(('dp', 'head'))
- grad_tokens: bfloat16 [24576, 1152], P(('dp', 'head'))
- grad_cond: float32 [96, 1152], P('dp')
- grad_w_ada: float32 [1152, 6912], P(None, 'head')
- grad_b_ada: float32 [6912], P('head')
- grad_w_qkv: float32 [1152, 3, 1152], P(None, None, 'head')
- grad_bias_qv: float32 [2, 1152], P(None, 'head')
- grad_w_proj: float32 [1152, 1152], P('head')
- grad_b_proj: float32 [1152], replicated
- grad_w_fc1: float32 [1152, 4608], P(None, 'head')
- grad_b_fc1: float32 [4608], P('head')
- grad_w_fc2: float32 [4608, 1152], P('head')
- grad_b_fc2: float32 [1152], replicated
The draws below stay inside these ranges and needn't reach their ends.
Inputs may be any that keep to these rules, and one draw needn't show every extreme that they name: `segment_ids`: each packed row of 2048 consecutive tokens is two halves of 1024 tokens, each either one segment or segments of 256 tokens. The ids of the tokens of index g of dp lie in g * 24 onward; a segment's id is that base plus (its first position within those tokens) // 256, so ids never fall and some slots name no token. In the last packed row of every index of dp the first half is one segment and the second half is split.
All inputs are finite; a program needn't handle non-finite values.
Results may differ from the reference program's by a relative error of at most 0.019.
The reference program's roundings to bfloat16 on the way count: a program that leaves them out, or rounds other values in their place, can miss the bound.
Values may be sent and summed in bfloat16 or wider, within the bound.
A program may use at most 320 MiB of HBM per device.

```python
import math
import jax
import jax.numpy as jnp
from jax import lax

D = 1152
HEADS = 16
HEAD_DIM = 72
FF = 4608
SHORT_SEQ = 256
LONG_SEQ = 1024
PACK = 2048
TOK_DEV = 6144
TOKENS = 24576
SEGS = 96


def draw_segment_ids(key, part):
    packed = TOKENS // PACK
    per_group = TOK_DEV // PACK
    slots_row = PACK // SHORT_SEQ
    per_half = LONG_SEQ // SHORT_SEQ
    single = jax.random.randint(key, (packed, 2), 0, 2)
    row_index = jnp.arange(packed)
    forced = row_index % per_group == per_group - 1
    single = jnp.where(forced[:, None], jnp.array([1, 0])[None, :], single)
    position = jnp.arange(PACK)
    half = position // LONG_SEQ
    small_slot = position % LONG_SEQ // SHORT_SEQ
    single_here = single[:, half]
    slot = half[None, :] * per_half + jnp.where(single_here == 1, 0, small_slot[None, :])
    group = row_index // per_group
    base = group * (TOK_DEV // SHORT_SEQ) + row_index % per_group * slots_row
    return (base[:, None] + slot).reshape(-1).astype(jnp.int32)


def levels(own_key, extent, pieces, least, high):
    loudness, own = 1.0, jax.random.fold_in(own_key, 6)
    for axis_at, shards_of in pieces:
        steps = jnp.exp(jax.random.uniform(jax.random.fold_in(own, axis_at), (shards_of,), jnp.float32, least / len(pieces), high / len(pieces)))
        loudness = loudness * jnp.repeat(steps, extent[axis_at] // shards_of).reshape([-1 if axis == axis_at else 1 for axis in range(len(extent))])
    return loudness


def bell_draw(key, shape, scale, most, pieces=(), kind=jnp.bfloat16):
    values = jax.random.normal(key, shape, jnp.float32) * scale
    if len(pieces) > 0:
        values = levels(key, shape, pieces, -0.22, 0.18) * values
    return jnp.clip(values, min=-most, max=most).astype(kind)


def setup_inputs(seed: int = 0) -> dict:
    seeds = jax.random.split(jax.random.key(seed), 15)
    return {
        "tokens": bell_draw(seeds[0], (TOKENS, D), 1.0, 6.0, ((0, 32),)),
        "segment_ids": draw_segment_ids(jax.random.fold_in(seeds[14], 71), 0),
        "cond": bell_draw(seeds[2], (SEGS, D), 1.0, 6.0, ((0, 4),), jnp.float32),
        "w_ada": bell_draw(seeds[3], (D, 6 * D), D ** -0.5, 0.1875, ((1, 8),)),
        "b_ada": bell_draw(seeds[4], (6 * D,), 0.3, 4.0, ((0, 8),)),
        "w_qkv": bell_draw(seeds[5], (D, 3, D), D ** -0.5, 0.1875, ((2, 8),)),
        "bias_qv": bell_draw(seeds[6], (2, D), 0.3, 4.0, ((1, 8),)),
        "w_proj": bell_draw(seeds[7], (D, D), (D // 16) ** -0.5, 0.75, ((0, 8),)),
        "b_proj": bell_draw(seeds[8], (D,), 0.3, 4.0),
        "w_fc1": bell_draw(seeds[9], (D, FF), D ** -0.5, 0.1875, ((1, 8),)),
        "b_fc1": bell_draw(seeds[10], (FF,), 0.3, 4.0, ((0, 8),)),
        "w_fc2": bell_draw(seeds[11], (FF, D), FF ** -0.5, 0.09375, ((0, 8),)),
        "b_fc2": bell_draw(seeds[12], (D,), 0.3, 4.0),
        "cotangent": bell_draw(seeds[13], (TOKENS, D), 1.0, 6.0, ((0, 32),)),
    }


@jax.custom_vjp
def low(v):
    return lax.optimization_barrier(v.astype(jnp.bfloat16)).astype(jnp.float32)

@jax.custom_vjp
def low_back(v):
    return v

def low_keep(v):
    return (low(v), None)

def low_pass(kept, grad):
    return (grad,)

def back_keep(v):
    return (v, None)

def back_low(kept, grad):
    return (low(grad),)
low.defvjp(low_keep, low_pass)
low_back.defvjp(back_keep, back_low)
norm_eps = 1e-06
top_precision = lax.Precision.HIGHEST

def dense(left, right):
    return jnp.dot(left, right, precision=top_precision, preferred_element_type=jnp.float32)

def layer_norm(values):
    centered = values - lax.optimization_barrier(jnp.mean(values, axis=-1, keepdims=True))
    return centered * lax.rsqrt(lax.optimization_barrier(jnp.mean(centered * centered, axis=-1, keepdims=True)) + norm_eps)

def row_layer(weights, modulation, token_row, ident_row):
    w_qkv, bias_qv, w_proj, b_proj, w_fc1, b_fc1, w_fc2, b_fc2 = weights
    per_token = modulation[ident_row]
    shift_a, scale_a, gate_a, shift_m, scale_m, gate_m = jnp.split(per_token, 6, axis=1)
    attn_in = low(layer_norm(token_row) * (1.0 + scale_a) + shift_a)
    zero_bias = jnp.zeros((D,), jnp.float32)
    qkv = dense(attn_in, w_qkv.reshape(D, 3 * D)) + jnp.concatenate([bias_qv[0], zero_bias, bias_qv[1]])
    query = low(low_back(qkv[:, :D])).reshape(PACK, HEADS, HEAD_DIM)
    keys = low(low_back(qkv[:, D:2 * D])).reshape(PACK, HEADS, HEAD_DIM)
    values = low(low_back(qkv[:, 2 * D:])).reshape(PACK, HEADS, HEAD_DIM)
    scale = 1.0 / math.sqrt(HEAD_DIM)
    scores = low_back(jnp.einsum('qhd,khd->hqk', query, keys, precision=top_precision) * scale)
    allowed = (ident_row[:, None] == ident_row[None, :])[None]
    probs = low(jax.nn.softmax(jnp.where(allowed, scores, -1e+30), axis=-1))
    mixed = jnp.einsum('hqk,khd->qhd', probs, values, precision=top_precision).reshape(PACK, D)
    mixed = low(low_back(mixed))
    branch_a = low_back(dense(mixed, w_proj) + b_proj)
    mid = token_row + gate_a * branch_a
    mlp_in = low(layer_norm(mid) * (1.0 + scale_m) + shift_m)
    pre = low_back(dense(mlp_in, w_fc1) + b_fc1)
    hidden = low(jax.nn.gelu(pre, approximate=True))
    branch_m = low_back(dense(hidden, w_fc2) + b_fc2)
    return mid + gate_m * branch_m

def reference(tokens, segment_ids, cond, w_ada, b_ada, w_qkv, bias_qv, w_proj, b_proj, w_fc1, b_fc1, w_fc2, b_fc2, cotangent):
    inputs = tuple((operand.astype(jnp.float32) for operand in (tokens, cond, w_ada, b_ada, w_qkv, bias_qv, w_proj, b_proj, w_fc1, b_fc1, w_fc2, b_fc2)))
    ident_rows = segment_ids.reshape(-1, PACK)

    def whole(resid, cond_in, ada_weight, ada_bias, *weights):
        modulation = dense(low(jax.nn.silu(cond_in)), ada_weight) + ada_bias

        def one_row(pair):
            return row_layer(weights, modulation, pair[0], pair[1])
        rows_out = lax.map(jax.checkpoint(one_row), (resid.reshape(-1, PACK, D), ident_rows))
        return rows_out.reshape(-1, D)
    output, pull = jax.vjp(whole, *inputs)
    grads = pull(cotangent.astype(jnp.float32))
    return (output.astype(jnp.bfloat16), grads[0].astype(jnp.bfloat16), grads[1], grads[2], grads[3], grads[4], grads[5], grads[6], grads[7], grads[8], grads[9], grads[10], grads[11])
```

```python
import functools
import math

import jax
import jax.numpy as jnp
from jax import lax
from jax.experimental import pallas as pl
from jax.experimental.pallas import tpu as pltpu
from jax.sharding import Mesh
from jax.sharding import PartitionSpec as P

HEAD_DIM = 72
LONG_SEQ = 1024
SHORT_SEQ = 256
LANES = 128
NORM_EPS = 1e-06
TOP = lax.Precision.HIGHEST
F32 = jnp.float32
BF16 = jnp.bfloat16

OUTER, CORE, PART, GROUP = "outer", "core", "part", "group"
DP = (OUTER, CORE)
HEAD = (PART, GROUP)
SPREAD = (CORE, PART, GROUP)
EVERY = (OUTER, CORE, PART, GROUP)

NT = (((1,), (1,)), ((), ()))
TN = (((0,), (0,)), ((), ()))


def layer_norm(values):
    centered = values - jnp.mean(values, axis=-1, keepdims=True)
    inverse = lax.rsqrt(jnp.mean(centered * centered, axis=-1, keepdims=True) + NORM_EPS)
    return (centered * inverse, inverse)


def norm_back(grad_normed, normed, inverse):
    mean_grad = jnp.mean(grad_normed, axis=-1, keepdims=True)
    mean_cross = jnp.mean(grad_normed * normed, axis=-1, keepdims=True)
    return inverse * (grad_normed - mean_grad - normed * mean_cross)


def head_columns(index, cols, offset):
    per_shard = cols // HEAD_DIM
    shard, within = index // per_shard, index % per_shard
    return shard * 3 * cols + offset * cols + within * HEAD_DIM


def attend_kernel(heads, cols, single_ref, qkv_ref, mix_ref, q_s, k_s, v_s, o_s):
    scale = 1.0 / math.sqrt(HEAD_DIM)
    units = LONG_SEQ // SHORT_SEQ
    pad = jnp.zeros((LONG_SEQ, LANES - HEAD_DIM), BF16)
    for h in range(heads):
        for offset, ref in enumerate((q_s, k_s, v_s)):
            at = head_columns(h, cols, offset)
            ref[h, :, :HEAD_DIM] = qkv_ref[:, at : at + HEAD_DIM]
            ref[h, :, HEAD_DIM:] = pad

    def attend_keys(h, rows, key_rows):
        scores = (
            lax.dot_general(q_s[h, rows], k_s[h, key_rows], NT, preferred_element_type=F32) * scale
        )
        weights = jnp.exp(scores - jnp.max(scores, axis=-1, keepdims=True))
        probs = weights * (1.0 / jnp.sum(weights, axis=-1, keepdims=True))
        o_s[h, rows] = jnp.dot(
            probs.astype(BF16), v_s[h, key_rows], preferred_element_type=F32
        ).astype(BF16)

    def step(i, carry):
        h = i // units
        rows = pl.ds(pl.multiple_of((i % units) * SHORT_SEQ, SHORT_SEQ), SHORT_SEQ)

        @pl.when(single_ref[pl.program_id(0)] == 1)
        def _():
            attend_keys(h, rows, slice(None))

        @pl.when(single_ref[pl.program_id(0)] == 0)
        def _():
            attend_keys(h, rows, rows)

        return carry

    lax.fori_loop(0, heads * units, step, 0)
    for h in range(heads):
        mix_ref[:, h * HEAD_DIM : (h + 1) * HEAD_DIM] = o_s[h, :, :HEAD_DIM]


def attend(single, qkv, heads, cols):
    rows, width = qkv.shape
    blocks = rows // LONG_SEQ
    return pl.pallas_call(
        functools.partial(attend_kernel, heads, cols),
        grid_spec=pltpu.PrefetchScalarGridSpec(
            num_scalar_prefetch=1,
            grid=(blocks,),
            in_specs=[pl.BlockSpec((LONG_SEQ, width), lambda b, s: (b, 0))],
            out_specs=pl.BlockSpec((LONG_SEQ, heads * HEAD_DIM), lambda b, s: (b, 0)),
            scratch_shapes=[pltpu.VMEM((heads, LONG_SEQ, LANES), BF16)] * 4,
        ),
        out_shape=jax.ShapeDtypeStruct((rows, heads * HEAD_DIM), BF16),
        cost_estimate=pl.CostEstimate(
            flops=4 * rows * LONG_SEQ * heads * LANES,
            bytes_accessed=2 * rows * (width + heads * HEAD_DIM),
            transcendentals=rows * LONG_SEQ * heads,
        ),
        name="attend",
    )(single, qkv)


def attend_back_kernel(
    heads, cols, single_ref, qkv_ref, grad_ref, out_ref, q_s, k_s, v_s, g_s, dq_s, dk_s, dv_s, kt_s
):
    scale = 1.0 / math.sqrt(HEAD_DIM)
    units = LONG_SEQ // SHORT_SEQ
    pad = jnp.zeros((LONG_SEQ, LANES - HEAD_DIM), BF16)
    for h in range(heads):
        for offset, ref in enumerate((q_s, k_s, v_s)):
            at = head_columns(h, cols, offset)
            ref[h, :, :HEAD_DIM] = qkv_ref[:, at : at + HEAD_DIM]
            ref[h, :, HEAD_DIM:] = pad
        g_s[h, :, :HEAD_DIM] = grad_ref[:, h * HEAD_DIM : (h + 1) * HEAD_DIM]
        g_s[h, :, HEAD_DIM:] = pad
        kt_s[h] = k_s[h].T
    is_single = single_ref[pl.program_id(0)] == 1

    def grads(h, rows, key_rows):
        q, g = q_s[h, rows], g_s[h, rows]
        k, v = k_s[h, key_rows], v_s[h, key_rows]
        scores = lax.dot_general(k, q, NT, preferred_element_type=F32) * scale
        weights = jnp.exp(scores - jnp.max(scores, axis=0, keepdims=True))
        probs = weights * (1.0 / jnp.sum(weights, axis=0, keepdims=True))
        grad_probs = lax.dot_general(v, g, NT, preferred_element_type=F32)
        inner = jnp.sum(probs * grad_probs, axis=0, keepdims=True)
        grad_scores = (probs * (grad_probs - inner)).astype(BF16)
        grad_v = jnp.dot(probs.astype(BF16), g, preferred_element_type=F32)
        grad_k = jnp.dot(grad_scores, q, preferred_element_type=F32)
        grad_q = jnp.dot(kt_s[h, :, key_rows], grad_scores, preferred_element_type=F32)
        dq_s[h, rows] = (grad_q.T * scale).astype(BF16)
        return grad_k, grad_v

    @pl.when(is_single)
    def _():
        dk_s[...] = jnp.zeros_like(dk_s)
        dv_s[...] = jnp.zeros_like(dv_s)

    def step(i, carry):
        h = i // units
        rows = pl.ds(pl.multiple_of((i % units) * SHORT_SEQ, SHORT_SEQ), SHORT_SEQ)

        @pl.when(is_single)
        def _():
            grad_k, grad_v = grads(h, rows, slice(None))
            dk_s[h] += grad_k
            dv_s[h] += grad_v

        @pl.when(jnp.logical_not(is_single))
        def _():
            grad_k, grad_v = grads(h, rows, rows)
            dk_s[h, rows] = grad_k
            dv_s[h, rows] = grad_v

        return carry

    lax.fori_loop(0, heads * units, step, 0)
    for h in range(heads):
        for offset, value in enumerate(
            (dq_s[h], (dk_s[h] * scale).astype(BF16), dv_s[h].astype(BF16))
        ):
            at = head_columns(h, cols, offset)
            out_ref[:, at : at + HEAD_DIM] = value[:, :HEAD_DIM]


def attend_back(single, qkv, grad_mix, heads, cols):
    rows, width = qkv.shape
    blocks = rows // LONG_SEQ
    low = pltpu.VMEM((heads, LONG_SEQ, LANES), BF16)
    wide = pltpu.VMEM((heads, LONG_SEQ, LANES), F32)
    return pl.pallas_call(
        functools.partial(attend_back_kernel, heads, cols),
        grid_spec=pltpu.PrefetchScalarGridSpec(
            num_scalar_prefetch=1,
            grid=(blocks,),
            in_specs=[
                pl.BlockSpec((LONG_SEQ, width), lambda b, s: (b, 0)),
                pl.BlockSpec((LONG_SEQ, heads * HEAD_DIM), lambda b, s: (b, 0)),
            ],
            out_specs=pl.BlockSpec((LONG_SEQ, width), lambda b, s: (b, 0)),
            scratch_shapes=[low] * 5 + [wide] * 2 + [pltpu.VMEM((heads, LANES, LONG_SEQ), BF16)],
        ),
        out_shape=jax.ShapeDtypeStruct((rows, width), BF16),
        cost_estimate=pl.CostEstimate(
            flops=10 * rows * LONG_SEQ * heads * LANES,
            bytes_accessed=2 * rows * (2 * width + heads * HEAD_DIM),
            transcendentals=rows * LONG_SEQ * heads,
        ),
        name="attend_back",
    )(single, qkv, grad_mix)


def mlp_kernel(x_ref, g_ref, w1_ref, w2_ref, b1_ref, out_ref, gin_ref, d1_ref, d2_ref, db_ref):
    @pl.when(pl.program_id(0) == 0)
    def _():
        out_ref[...] = jnp.zeros_like(out_ref)
        gin_ref[...] = jnp.zeros_like(gin_ref)

    root = math.sqrt(2.0 / math.pi)
    x, g, w1, w2 = x_ref[...], g_ref[...], w1_ref[...], w2_ref[...]
    pre = lax.dot_general(x, w1, NT, preferred_element_type=F32) + b1_ref[0]
    grad_hidden = lax.dot_general(g, w2, NT, preferred_element_type=F32)
    square = pre * pre
    bent = jnp.tanh(root * (pre * (1.0 + 0.044715 * square)))
    half = 0.5 * (1.0 + bent)
    slope = half + (0.5 * root) * pre * (1.0 - bent * bent) * (1.0 + (3 * 0.044715) * square)
    hidden = (pre * half).astype(BF16)
    grad_pre = (grad_hidden * slope).astype(BF16)
    out_ref[...] += jnp.dot(hidden, w2, preferred_element_type=F32)
    gin_ref[...] += jnp.dot(grad_pre, w1, preferred_element_type=F32)
    d2_ref[...] = lax.dot_general(hidden, g, TN, preferred_element_type=F32).astype(BF16)
    d1_ref[...] = lax.dot_general(grad_pre, x, TN, preferred_element_type=F32).astype(BF16)
    db_ref[0] = jnp.sum(grad_pre.astype(F32), axis=0, keepdims=True)


def mlp(x, g, w1, w2, b1):
    rows, width = x.shape
    units = w1.shape[0]
    tile = next(t for t in (512, 256, 128) if units % t == 0)
    tiles = units // tile
    whole = pl.BlockSpec((rows, width), lambda f: (0, 0))
    piece = pl.BlockSpec((tile, width), lambda f: (f, 0))
    line = pl.BlockSpec((1, 1, tile), lambda f: (f, 0, 0))
    return pl.pallas_call(
        mlp_kernel,
        grid=(tiles,),
        in_specs=[whole, whole, piece, piece, line],
        out_specs=[whole, whole, piece, piece, line],
        out_shape=[
            jax.ShapeDtypeStruct((rows, width), F32),
            jax.ShapeDtypeStruct((rows, width), F32),
            jax.ShapeDtypeStruct((units, width), BF16),
            jax.ShapeDtypeStruct((units, width), BF16),
            jax.ShapeDtypeStruct((tiles, 1, tile), F32),
        ],
        cost_estimate=pl.CostEstimate(
            flops=12 * rows * width * units,
            bytes_accessed=8 * units * width + 12 * rows * width,
            transcendentals=rows * units,
        ),
        name="mlp",
    )(x, g, w1, w2, b1.reshape(tiles, 1, tile))


def xor_pairs(size, mask):
    return [(i, i ^ mask) for i in range(size)]


def swap(value, axis, size, mask):
    return lax.ppermute(value, axis, xor_pairs(size, mask))


def gather_group(own, size):
    rows = own.shape[0]
    me = lax.axis_index(GROUP)
    if size != 4:
        return lax.all_gather(own, GROUP, axis=0, tiled=True)
    half = rows // 2
    near = swap(own, GROUP, 4, 1)
    far = swap(own, GROUP, 4, 2)
    upper = swap(far[:half], GROUP, 4, 1)
    lower = swap(near[half:], GROUP, 4, 2)
    whole = jnp.zeros((4 * rows, own.shape[1]), own.dtype)
    for mask, at, piece in (
        (0, 0, own),
        (1, 0, near),
        (2, 0, far),
        (3, 0, upper),
        (3, half, lower),
    ):
        start = jnp.bitwise_xor(me, mask) * rows + at
        whole = lax.dynamic_update_slice_in_dim(whole, piece, start, 0)
    return whole


def scatter_group(partial, size):
    if size != 4:
        return lax.psum_scatter(partial, GROUP, scatter_dimension=0, tiled=True).astype(F32)
    rows = partial.shape[0] // 4
    half = rows // 2
    me = lax.axis_index(GROUP)

    def piece(mask, at):
        start = jnp.bitwise_xor(me, mask) * rows + at
        return lax.dynamic_slice_in_dim(partial, start, half)

    upper = swap(jnp.stack([piece(1, 0), piece(3, 0)]), GROUP, 4, 1)
    lower = swap(jnp.stack([piece(2, half), piece(3, half)]), GROUP, 4, 2)
    upper_far = swap((piece(2, 0).astype(F32) + upper[1].astype(F32)).astype(BF16), GROUP, 4, 2)
    lower_far = swap((piece(1, half).astype(F32) + lower[1].astype(F32)).astype(BF16), GROUP, 4, 1)
    return jnp.concatenate(
        [
            piece(0, 0).astype(F32) + upper[0].astype(F32) + upper_far.astype(F32),
            piece(0, half).astype(F32) + lower[0].astype(F32) + lower_far.astype(F32),
        ]
    )


def sum_outer(value, size):
    total = value.astype(F32)
    if size & (size - 1):
        return lax.psum(value, OUTER).astype(F32)
    mask = 1
    while mask < size:
        total = total + swap(total.astype(BF16), OUTER, size, mask).astype(F32)
        total = total if mask * 2 >= size else total.astype(BF16).astype(F32)
        mask *= 2
    return total


def join_cores(own):
    own = own.astype(BF16)
    other = swap(own, CORE, 2, 1)
    first = lax.axis_index(CORE) == 0
    return jnp.concatenate([jnp.where(first, own, other), jnp.where(first, other, own)])


def core_half(value):
    half = value.shape[0] // 2
    return lax.dynamic_slice_in_dim(value, lax.axis_index(CORE) * half, half)


def local(
    sizes,
    tokens,
    segment_ids,
    cond,
    w_ada,
    b_ada,
    w_qkv,
    bias_qv,
    w_proj,
    b_proj,
    w_fc1,
    b_fc1,
    w_fc2,
    b_fc2,
    cotangent,
):
    outer_size, part_size, group_size = sizes
    head_size = part_size * group_size
    rows, width = tokens.shape
    slots = cond.shape[0]
    cols = w_qkv.shape[2]
    ada_cols = w_ada.shape[1]
    ff_here = w_fc1.shape[1]
    unit = math.gcd(rows, SHORT_SEQ)
    units = rows // unit
    heads = part_size * cols // HEAD_DIM
    head_at = lax.axis_index(HEAD)

    proj_half, fc1_half = cols // 2, ff_here // 2
    bias_row = jnp.pad(core_half(b_fc1)[None, :], ((0, 0), (0, width - fc1_half)))
    proj_sent = jnp.concatenate([core_half(w_proj), bias_row])
    proj_rows = lax.all_gather(proj_sent, SPREAD, axis=0)
    proj_rows = proj_rows.reshape(2 * head_size, proj_half + 1, width)
    proj_full = proj_rows[:, :proj_half].reshape(-1, width)
    bias_fc1 = proj_rows[:, proj_half, :fc1_half].reshape(-1).astype(F32)
    fc1_full = lax.all_gather(core_half(w_fc1.T), SPREAD, axis=0, tiled=True)
    fc2_full = lax.all_gather(core_half(w_fc2), SPREAD, axis=0, tiled=True)
    qkv_own = jnp.transpose(w_qkv, (1, 2, 0)).reshape(3 * cols, width)
    if part_size == 2:
        qkv_other = swap(qkv_own, PART, 2, 1)
        low_part = lax.axis_index(PART) == 0
        qkv_weight = jnp.concatenate(
            [jnp.where(low_part, qkv_own, qkv_other), jnp.where(low_part, qkv_other, qkv_own)]
        )
    else:
        qkv_weight = lax.all_gather(qkv_own, PART, axis=0, tiled=True)
    bias_own = jnp.concatenate([bias_qv[0], jnp.zeros((cols,), bias_qv.dtype), bias_qv[1]])
    qkv_bias = lax.all_gather(bias_own, PART, axis=0, tiled=True).astype(F32)

    unit_ids = segment_ids[::unit] - lax.axis_index(DP) * slots
    pick = (unit_ids[:, None] == jnp.arange(slots, dtype=jnp.int32)[None, :]).astype(F32)
    cond_act, silu_back = jax.vjp(jax.nn.silu, cond)
    cond_low = cond_act.astype(BF16)
    cond_all = lax.all_gather(cond_low, DP, axis=0, tiled=True)
    mod_part = jnp.dot(cond_low, w_ada, preferred_element_type=F32) + b_ada.astype(F32)
    mod_sent = jnp.dot(pick, mod_part, precision=TOP).reshape(head_size, units, ada_cols)
    mod_got = lax.all_to_all(mod_sent, HEAD, split_axis=0, concat_axis=0, tiled=True)
    modulation = jnp.transpose(mod_got, (1, 0, 2)).reshape(units, 6, 1, width)
    shift_a, scale_a, gate_a, shift_m, scale_m, gate_m = [modulation[:, i] for i in range(6)]

    def by_unit(value):
        return value.reshape(units, unit, width)

    def flat(value):
        return value.reshape(rows, width)

    resid = by_unit(tokens.astype(F32))
    normed_a, inverse_a = layer_norm(resid)
    attn_in = flat((normed_a * (1.0 + scale_a) + shift_a).astype(BF16))
    gathered = gather_group(attn_in, group_size)
    qkv = (lax.dot_general(gathered, qkv_weight, NT, preferred_element_type=F32) + qkv_bias).astype(
        BF16
    )
    blocks = gathered.shape[0] // LONG_SEQ
    first = lax.axis_index(PART) * gathered.shape[0] + jnp.arange(blocks) * LONG_SEQ
    single = (segment_ids[first] == segment_ids[first + SHORT_SEQ]).astype(jnp.int32)
    mix_part = attend(single, qkv, heads, cols)
    mix_got = lax.all_to_all(
        mix_part.reshape(group_size, rows, heads * HEAD_DIM), GROUP, split_axis=0, concat_axis=0
    )
    mix_got = mix_got.reshape(group_size, rows, part_size, 2, proj_half)
    mix = jnp.transpose(mix_got, (1, 3, 2, 0, 4)).reshape(rows, width)
    branch_a = by_unit(
        jnp.dot(mix, proj_full, preferred_element_type=F32) + b_proj.astype(F32)
    )
    mid = resid + gate_a * branch_a
    normed_m, inverse_m = layer_norm(mid)
    mlp_in = flat((normed_m * (1.0 + scale_m) + shift_m).astype(BF16))
    cotan = by_unit(cotangent.astype(F32))
    grad_branch_m = flat((gate_m * cotan).astype(BF16))
    branch_m, grad_mlp_in, grad_fc1, grad_fc2, grad_b1 = mlp(
        mlp_in, grad_branch_m, fc1_full, fc2_full, bias_fc1
    )
    grad_fc2 = lax.psum_scatter(grad_fc2, SPREAD, scatter_dimension=0, tiled=True)
    grad_fc1 = lax.psum_scatter(grad_fc1, SPREAD, scatter_dimension=0, tiled=True)
    branch_m = by_unit(branch_m) + b_fc2.astype(F32)
    grad_mlp_in = by_unit(grad_mlp_in)
    output = flat((mid + gate_m * branch_m).astype(BF16))
    grad_mid = cotan + norm_back(grad_mlp_in * (1.0 + scale_m), normed_m, inverse_m)
    grad_branch_a = flat((gate_a * grad_mid).astype(BF16))
    grad_mix = lax.dot_general(grad_branch_a, proj_full, NT, preferred_element_type=F32)
    grad_mix = grad_mix.astype(BF16).reshape(rows, 2, part_size, group_size, proj_half)
    grad_mix = jnp.transpose(grad_mix, (3, 0, 2, 1, 4)).reshape(group_size, rows, -1)
    grad_mix = lax.all_to_all(grad_mix, GROUP, split_axis=0, concat_axis=0)
    grad_proj = lax.dot_general(mix, grad_branch_a, TN, preferred_element_type=F32).astype(BF16)
    b1_row = jnp.pad(
        grad_b1.reshape(2 * head_size, 1, fc1_half).astype(BF16),
        ((0, 0), (0, 0), (0, width - fc1_half)),
    )
    grad_proj = jnp.concatenate([grad_proj.reshape(2 * head_size, proj_half, width), b1_row], axis=1)
    grad_proj = lax.psum_scatter(grad_proj, SPREAD, scatter_dimension=0, tiled=True)[0]
    grad_qkv = attend_back(single, qkv, grad_mix.reshape(-1, heads * HEAD_DIM), heads, cols)
    attn_grad_part = jnp.dot(grad_qkv, qkv_weight, preferred_element_type=F32).astype(BF16)
    grad_attn_in = by_unit(scatter_group(attn_grad_part, group_size))

    grad_w_qkv = lax.dot_general(grad_qkv, gathered, TN, preferred_element_type=F32)
    grad_bias = jnp.sum(grad_qkv.astype(F32), axis=0)
    bias_rows = jnp.pad(grad_bias.reshape(part_size, 1, 3 * cols), ((0, 0), (0, 0), (0, width - 3 * cols)))
    pad_rows = jnp.zeros((part_size, 15, width), F32)
    grad_w_qkv = jnp.concatenate(
        [grad_w_qkv.reshape(part_size, 3 * cols, width), bias_rows, pad_rows], axis=1
    ).astype(BF16)
    if part_size == 2:
        mine, theirs = grad_w_qkv[0], grad_w_qkv[1]
        low_part = lax.axis_index(PART) == 0
        kept = jnp.where(low_part, mine, theirs)
        sent = jnp.where(low_part, theirs, mine)
        grad_w_qkv = kept.astype(F32) + swap(sent, PART, 2, 1).astype(F32)
    else:
        grad_w_qkv = lax.psum_scatter(
            grad_w_qkv, PART, scatter_dimension=0, tiled=True
        )[0].astype(F32)
    half = grad_w_qkv.shape[0] // 2
    other = swap(
        lax.dynamic_slice_in_dim(grad_w_qkv, (1 - lax.axis_index(CORE)) * half, half).astype(BF16),
        CORE,
        2,
        1,
    )
    grad_w_qkv = (core_half(grad_w_qkv) + other.astype(F32)).astype(BF16)
    grad_w_qkv = join_cores(sum_outer(grad_w_qkv, outer_size)).astype(F32)
    grad_bias = grad_w_qkv[3 * cols, : 3 * cols]
    grad_bias_qv = jnp.stack([grad_bias[:cols], grad_bias[2 * cols :]])
    grad_w_qkv = jnp.transpose(grad_w_qkv[: 3 * cols].reshape(3, cols, width), (2, 0, 1))

    grad_fc2 = join_cores(sum_outer(grad_fc2, outer_size)).astype(F32)
    grad_fc1 = join_cores(sum_outer(grad_fc1, outer_size)).astype(F32).T
    grad_proj = join_cores(sum_outer(grad_proj, outer_size)).astype(F32)
    grad_proj = grad_proj.reshape(2, proj_half + 1, width)
    grad_b1 = grad_proj[:, proj_half, :fc1_half].reshape(-1)
    grad_proj = grad_proj[:, :proj_half].reshape(cols, width)

    grad_tokens = flat(
        (grad_mid + norm_back(grad_attn_in * (1.0 + scale_a), normed_a, inverse_a)).astype(BF16)
    )
    unit_grad = jnp.concatenate(
        [
            jnp.sum(value, axis=1)
            for value in (
                grad_attn_in,
                grad_attn_in * normed_a,
                grad_mid * branch_a,
                grad_mlp_in,
                grad_mlp_in * normed_m,
                cotan * branch_m,
            )
        ],
        axis=1,
    )
    unit_grad = jnp.transpose(unit_grad.reshape(units, head_size, ada_cols), (1, 0, 2))
    unit_grad = lax.all_to_all(unit_grad, HEAD, split_axis=0, concat_axis=0, tiled=True)
    grad_mod = lax.dot_general(
        pick, unit_grad.reshape(head_size * units, ada_cols), TN, precision=TOP
    )
    grad_mod_all = lax.all_gather(grad_mod, DP, axis=0, tiled=True)
    grad_w_ada = lax.dot_general(cond_all.astype(F32), grad_mod_all, TN, precision=TOP)
    grad_b_ada = jnp.sum(grad_mod_all, axis=0)
    grad_cond_part = lax.dot_general(grad_mod, w_ada.astype(F32), NT, precision=TOP)
    grad_cond = silu_back(lax.psum(grad_cond_part, HEAD))[0]
    bias_parts = jnp.stack(
        [
            jnp.sum(grad_branch_a.astype(F32), axis=0),
            jnp.sum(grad_branch_m.astype(F32), axis=0),
        ]
    )
    bias_sums = lax.psum(bias_parts, EVERY)
    return (
        output,
        grad_tokens,
        grad_cond,
        grad_w_ada,
        grad_b_ada,
        grad_w_qkv,
        grad_bias_qv,
        grad_proj,
        bias_sums[0],
        grad_fc1,
        grad_b1,
        grad_fc2,
        bias_sums[1],
    )


def solution(mesh):
    dp_size, head_size = mesh.shape["dp"], mesh.shape["head"]

    def run(*arrays):
        rows = arrays[0].shape[0] // (dp_size * head_size)
        group_size = math.lcm(rows, LONG_SEQ) // rows
        sizes = (dp_size // 2, head_size // group_size, group_size)
        finer = Mesh(
            mesh.devices.reshape(sizes[0], 2, sizes[1], sizes[2]), (OUTER, CORE, PART, GROUP)
        )
        placed = (
            P(EVERY, None),
            P(DP),
            P(DP, None),
            P(None, HEAD),
            P(HEAD),
            P(None, None, HEAD),
            P(None, HEAD),
            P(HEAD, None),
            P(),
            P(None, HEAD),
            P(HEAD),
            P(HEAD, None),
            P(),
            P(EVERY, None),
        )
        results = (
            P(EVERY, None),
            P(EVERY, None),
            P(DP, None),
            P(None, HEAD),
            P(HEAD),
            P(None, None, HEAD),
            P(None, HEAD),
            P(HEAD, None),
            P(),
            P(None, HEAD),
            P(HEAD),
            P(HEAD, None),
            P(),
        )
        return jax.shard_map(
            functools.partial(local, sizes),
            mesh=finer,
            in_specs=placed,
            out_specs=results,
            check_vma=False,
        )(*arrays)

    return run
```

```python
import functools
import math

import jax
import jax.numpy as jnp
from jax import lax
from jax.experimental import pallas as pl
from jax.experimental.pallas import tpu as pltpu
from jax.sharding import Mesh
from jax.sharding import PartitionSpec as P

HEAD_DIM = 72
LONG_SEQ = 1024
SHORT_SEQ = 256
LANES = 128
NORM_EPS = 1e-06
TOP = lax.Precision.HIGHEST
F32 = jnp.float32
BF16 = jnp.bfloat16

OUTER, CORE, PART, GROUP = "outer", "core", "part", "group"
DP = (OUTER, CORE)
HEAD = (PART, GROUP)
SPREAD = (CORE, PART, GROUP)
EVERY = (OUTER, CORE, PART, GROUP)

NT = (((1,), (1,)), ((), ()))
TN = (((0,), (0,)), ((), ()))


def layer_norm(values):
    centered = values - jnp.mean(values, axis=-1, keepdims=True)
    inverse = lax.rsqrt(jnp.mean(centered * centered, axis=-1, keepdims=True) + NORM_EPS)
    return (centered * inverse, inverse)


def norm_back(grad_normed, normed, inverse):
    mean_grad = jnp.mean(grad_normed, axis=-1, keepdims=True)
    mean_cross = jnp.mean(grad_normed * normed, axis=-1, keepdims=True)
    return inverse * (grad_normed - mean_grad - normed * mean_cross)


def head_columns(index, cols, offset):
    per_shard = cols // HEAD_DIM
    shard, within = index // per_shard, index % per_shard
    return shard * 3 * cols + offset * cols + within * HEAD_DIM


def attend_kernel(heads, cols, single_ref, qkv_ref, mix_ref, q_s, k_s, v_s, o_s):
    scale = 1.0 / math.sqrt(HEAD_DIM)
    units = LONG_SEQ // SHORT_SEQ
    pad = jnp.zeros((LONG_SEQ, LANES - HEAD_DIM), BF16)
    for h in range(heads):
        for offset, ref in enumerate((q_s, k_s, v_s)):
            at = head_columns(h, cols, offset)
            ref[h, :, :HEAD_DIM] = qkv_ref[:, at : at + HEAD_DIM]
            ref[h, :, HEAD_DIM:] = pad

    def attend_keys(h, rows, key_rows):
        scores = (
            lax.dot_general(q_s[h, rows], k_s[h, key_rows], NT, preferred_element_type=F32) * scale
        )
        weights = jnp.exp(scores - jnp.max(scores, axis=-1, keepdims=True))
        probs = weights * (1.0 / jnp.sum(weights, axis=-1, keepdims=True))
        o_s[h, rows] = jnp.dot(
            probs.astype(BF16), v_s[h, key_rows], preferred_element_type=F32
        ).astype(BF16)

    def step(i, carry):
        h = i // units
        rows = pl.ds(pl.multiple_of((i % units) * SHORT_SEQ, SHORT_SEQ), SHORT_SEQ)

        @pl.when(single_ref[pl.program_id(0)] == 1)
        def _():
            attend_keys(h, rows, slice(None))

        @pl.when(single_ref[pl.program_id(0)] == 0)
        def _():
            attend_keys(h, rows, rows)

        return carry

    lax.fori_loop(0, heads * units, step, 0)
    for h in range(heads):
        mix_ref[:, h * HEAD_DIM : (h + 1) * HEAD_DIM] = o_s[h, :, :HEAD_DIM]


def attend(single, qkv, heads, cols):
    rows, width = qkv.shape
    blocks = rows // LONG_SEQ
    return pl.pallas_call(
        functools.partial(attend_kernel, heads, cols),
        grid_spec=pltpu.PrefetchScalarGridSpec(
            num_scalar_prefetch=1,
            grid=(blocks,),
            in_specs=[pl.BlockSpec((LONG_SEQ, width), lambda b, s: (b, 0))],
            out_specs=pl.BlockSpec((LONG_SEQ, heads * HEAD_DIM), lambda b, s: (b, 0)),
            scratch_shapes=[pltpu.VMEM((heads, LONG_SEQ, LANES), BF16)] * 4,
        ),
        out_shape=jax.ShapeDtypeStruct((rows, heads * HEAD_DIM), BF16),
        cost_estimate=pl.CostEstimate(
            flops=4 * rows * LONG_SEQ * heads * LANES,
            bytes_accessed=2 * rows * (width + heads * HEAD_DIM),
            transcendentals=rows * LONG_SEQ * heads,
        ),
        name="attend",
    )(single, qkv)


def attend_back_kernel(
    heads, cols, single_ref, qkv_ref, grad_ref, out_ref, q_s, k_s, v_s, g_s, dq_s, dk_s, dv_s, kt_s
):
    scale = 1.0 / math.sqrt(HEAD_DIM)
    units = LONG_SEQ // SHORT_SEQ
    pad = jnp.zeros((LONG_SEQ, LANES - HEAD_DIM), BF16)
    for h in range(heads):
        for offset, ref in enumerate((q_s, k_s, v_s)):
            at = head_columns(h, cols, offset)
            ref[h, :, :HEAD_DIM] = qkv_ref[:, at : at + HEAD_DIM]
            ref[h, :, HEAD_DIM:] = pad
        g_s[h, :, :HEAD_DIM] = grad_ref[:, h * HEAD_DIM : (h + 1) * HEAD_DIM]
        g_s[h, :, HEAD_DIM:] = pad
        kt_s[h] = k_s[h].T
    is_single = single_ref[pl.program_id(0)] == 1

    def grads(h, rows, key_rows):
        q, g = q_s[h, rows], g_s[h, rows]
        k, v = k_s[h, key_rows], v_s[h, key_rows]
        scores = lax.dot_general(k, q, NT, preferred_element_type=F32) * scale
        weights = jnp.exp(scores - jnp.max(scores, axis=0, keepdims=True))
        probs = weights * (1.0 / jnp.sum(weights, axis=0, keepdims=True))
        grad_probs = lax.dot_general(v, g, NT, preferred_element_type=F32)
        inner = jnp.sum(probs * grad_probs, axis=0, keepdims=True)
        grad_scores = (probs * (grad_probs - inner)).astype(BF16)
        grad_v = jnp.dot(probs.astype(BF16), g, preferred_element_type=F32)
        grad_k = jnp.dot(grad_scores, q, preferred_element_type=F32)
        grad_q = jnp.dot(kt_s[h, :, key_rows], grad_scores, preferred_element_type=F32)
        dq_s[h, rows] = (grad_q.T * scale).astype(BF16)
        return grad_k, grad_v

    @pl.when(is_single)
    def _():
        dk_s[...] = jnp.zeros_like(dk_s)
        dv_s[...] = jnp.zeros_like(dv_s)

    def step(i, carry):
        h = i // units
        rows = pl.ds(pl.multiple_of((i % units) * SHORT_SEQ, SHORT_SEQ), SHORT_SEQ)

        @pl.when(is_single)
        def _():
            grad_k, grad_v = grads(h, rows, slice(None))
            dk_s[h] += grad_k
            dv_s[h] += grad_v

        @pl.when(jnp.logical_not(is_single))
        def _():
            grad_k, grad_v = grads(h, rows, rows)
            dk_s[h, rows] = grad_k
            dv_s[h, rows] = grad_v

        return carry

    lax.fori_loop(0, heads * units, step, 0)
    for h in range(heads):
        for offset, value in enumerate(
            (dq_s[h], (dk_s[h] * scale).astype(BF16), dv_s[h].astype(BF16))
        ):
            at = head_columns(h, cols, offset)
            out_ref[:, at : at + HEAD_DIM] = value[:, :HEAD_DIM]


def attend_back(single, qkv, grad_mix, heads, cols):
    rows, width = qkv.shape
    blocks = rows // LONG_SEQ
    low = pltpu.VMEM((heads, LONG_SEQ, LANES), BF16)
    wide = pltpu.VMEM((heads, LONG_SEQ, LANES), F32)
    return pl.pallas_call(
        functools.partial(attend_back_kernel, heads, cols),
        grid_spec=pltpu.PrefetchScalarGridSpec(
            num_scalar_prefetch=1,
            grid=(blocks,),
            in_specs=[
                pl.BlockSpec((LONG_SEQ, width), lambda b, s: (b, 0)),
                pl.BlockSpec((LONG_SEQ, heads * HEAD_DIM), lambda b, s: (b, 0)),
            ],
            out_specs=pl.BlockSpec((LONG_SEQ, width), lambda b, s: (b, 0)),
            scratch_shapes=[low] * 5 + [wide] * 2 + [pltpu.VMEM((heads, LANES, LONG_SEQ), BF16)],
        ),
        out_shape=jax.ShapeDtypeStruct((rows, width), BF16),
        cost_estimate=pl.CostEstimate(
            flops=10 * rows * LONG_SEQ * heads * LANES,
            bytes_accessed=2 * rows * (2 * width + heads * HEAD_DIM),
            transcendentals=rows * LONG_SEQ * heads,
        ),
        name="attend_back",
    )(single, qkv, grad_mix)


def mlp_kernel(x_ref, g_ref, w1_ref, w2_ref, b1_ref, out_ref, gin_ref, d1_ref, d2_ref, db_ref):
    @pl.when(pl.program_id(0) == 0)
    def _():
        out_ref[...] = jnp.zeros_like(out_ref)
        gin_ref[...] = jnp.zeros_like(gin_ref)

    root = math.sqrt(2.0 / math.pi)
    x, g, w1, w2 = x_ref[...], g_ref[...], w1_ref[...], w2_ref[...]
    pre = lax.dot_general(x, w1, NT, preferred_element_type=F32) + b1_ref[0]
    grad_hidden = lax.dot_general(g, w2, NT, preferred_element_type=F32)
    square = pre * pre
    bent = jnp.tanh(root * (pre * (1.0 + 0.044715 * square)))
    half = 0.5 * (1.0 + bent)
    slope = half + (0.5 * root) * pre * (1.0 - bent * bent) * (1.0 + (3 * 0.044715) * square)
    hidden = (pre * half).astype(BF16)
    grad_pre = (grad_hidden * slope).astype(BF16)
    out_ref[...] += jnp.dot(hidden, w2, preferred_element_type=F32)
    gin_ref[...] += jnp.dot(grad_pre, w1, preferred_element_type=F32)
    d2_ref[...] = lax.dot_general(hidden, g, TN, preferred_element_type=F32).astype(BF16)
    d1_ref[...] = lax.dot_general(grad_pre, x, TN, preferred_element_type=F32).astype(BF16)
    db_ref[0] = jnp.sum(grad_pre.astype(F32), axis=0, keepdims=True)


def mlp(x, g, w1, w2, b1):
    rows, width = x.shape
    units = w1.shape[0]
    tile = next(t for t in (512, 256, 128) if units % t == 0)
    tiles = units // tile
    whole = pl.BlockSpec((rows, width), lambda f: (0, 0))
    piece = pl.BlockSpec((tile, width), lambda f: (f, 0))
    line = pl.BlockSpec((1, 1, tile), lambda f: (f, 0, 0))
    return pl.pallas_call(
        mlp_kernel,
        grid=(tiles,),
        in_specs=[whole, whole, piece, piece, line],
        out_specs=[whole, whole, piece, piece, line],
        out_shape=[
            jax.ShapeDtypeStruct((rows, width), F32),
            jax.ShapeDtypeStruct((rows, width), F32),
            jax.ShapeDtypeStruct((units, width), BF16),
            jax.ShapeDtypeStruct((units, width), BF16),
            jax.ShapeDtypeStruct((tiles, 1, tile), F32),
        ],
        cost_estimate=pl.CostEstimate(
            flops=12 * rows * width * units,
            bytes_accessed=8 * units * width + 12 * rows * width,
            transcendentals=rows * units,
        ),
        name="mlp",
    )(x, g, w1, w2, b1.reshape(tiles, 1, tile))


def xor_pairs(size, mask):
    return [(i, i ^ mask) for i in range(size)]


def swap(value, axis, size, mask):
    return lax.ppermute(value, axis, xor_pairs(size, mask))


def gather_group(own, size):
    rows = own.shape[0]
    me = lax.axis_index(GROUP)
    if size != 4:
        return lax.all_gather(own, GROUP, axis=0, tiled=True)
    half = rows // 2
    near = swap(own, GROUP, 4, 1)
    far = swap(own, GROUP, 4, 2)
    upper = swap(far[:half], GROUP, 4, 1)
    lower = swap(near[half:], GROUP, 4, 2)
    whole = jnp.zeros((4 * rows, own.shape[1]), own.dtype)
    for mask, at, piece in (
        (0, 0, own),
        (1, 0, near),
        (2, 0, far),
        (3, 0, upper),
        (3, half, lower),
    ):
        start = jnp.bitwise_xor(me, mask) * rows + at
        whole = lax.dynamic_update_slice_in_dim(whole, piece, start, 0)
    return whole


def scatter_group(partial, size):
    if size != 4:
        return lax.psum_scatter(partial, GROUP, scatter_dimension=0, tiled=True).astype(F32)
    rows = partial.shape[0] // 4
    half = rows // 2
    me = lax.axis_index(GROUP)

    def piece(mask, at):
        start = jnp.bitwise_xor(me, mask) * rows + at
        return lax.dynamic_slice_in_dim(partial, start, half)

    upper = swap(jnp.stack([piece(1, 0), piece(3, 0)]), GROUP, 4, 1)
    lower = swap(jnp.stack([piece(2, half), piece(3, half)]), GROUP, 4, 2)
    upper_far = swap((piece(2, 0).astype(F32) + upper[1].astype(F32)).astype(BF16), GROUP, 4, 2)
    lower_far = swap((piece(1, half).astype(F32) + lower[1].astype(F32)).astype(BF16), GROUP, 4, 1)
    return jnp.concatenate(
        [
            piece(0, 0).astype(F32) + upper[0].astype(F32) + upper_far.astype(F32),
            piece(0, half).astype(F32) + lower[0].astype(F32) + lower_far.astype(F32),
        ]
    )


def powers(size):
    return [1 << b for b in range(size.bit_length() - 1)] if size & (size - 1) == 0 else None


def sum_axis(value, axis, size):
    masks = powers(size)
    if masks is None:
        return lax.psum(value, axis)
    for mask in masks:
        value = value + swap(value, axis, size, mask)
    return value


def gather_axis(value, axis, size):
    masks = powers(size)
    if masks is None:
        return lax.all_gather(value, axis, axis=0, tiled=True)
    me = lax.axis_index(axis)
    for mask in masks:
        other = swap(value, axis, size, mask)
        first = jnp.bitwise_and(me, mask) == 0
        value = jnp.concatenate(
            [jnp.where(first, value, other), jnp.where(first, other, value)], axis=0
        )
    return value


def sum_outer(value, size):
    total = value.astype(F32)
    masks = powers(size)
    if masks is None:
        return lax.psum(value, OUTER).astype(F32)
    for mask in masks:
        low = total.astype(BF16)
        total = low.astype(F32) + swap(low, OUTER, size, mask).astype(F32)
    return total


def sum_cores(value):
    half = value.shape[0] // 2
    sent = lax.dynamic_slice_in_dim(value, (1 - lax.axis_index(CORE)) * half, half)
    got = swap(sent.astype(BF16), CORE, 2, 1)
    return core_half(value).astype(F32) + got.astype(F32)


def join_cores(own):
    own = own.astype(BF16)
    other = swap(own, CORE, 2, 1)
    first = lax.axis_index(CORE) == 0
    return jnp.concatenate([jnp.where(first, own, other), jnp.where(first, other, own)])


def scatter_weight(value):
    value = sum_cores(value).astype(BF16)
    return lax.psum_scatter(value, HEAD, scatter_dimension=0, tiled=True)


def core_half(value):
    half = value.shape[0] // 2
    return lax.dynamic_slice_in_dim(value, lax.axis_index(CORE) * half, half)


def spread_row(row, copies, width):
    row = jnp.pad(row, (0, width - row.shape[0]))
    return jnp.broadcast_to(row, (copies, 1, width))


def local(
    sizes,
    tokens,
    segment_ids,
    cond,
    w_ada,
    b_ada,
    w_qkv,
    bias_qv,
    w_proj,
    b_proj,
    w_fc1,
    b_fc1,
    w_fc2,
    b_fc2,
    cotangent,
):
    outer_size, part_size, group_size = sizes
    head_size = part_size * group_size
    rows, width = tokens.shape
    slots = cond.shape[0]
    cols = w_qkv.shape[2]
    ada_cols = w_ada.shape[1]
    ff_here = w_fc1.shape[1]
    unit = math.gcd(rows, SHORT_SEQ)
    units = rows // unit
    heads = part_size * cols // HEAD_DIM
    head_at = lax.axis_index(HEAD)

    proj_half = cols // 2
    proj_full = lax.all_gather(core_half(w_proj), SPREAD, axis=0, tiled=True)
    fc1_full = lax.all_gather(core_half(w_fc1.T), SPREAD, axis=0, tiled=True)
    fc2_full = lax.all_gather(core_half(w_fc2), SPREAD, axis=0, tiled=True)
    qkv_own = jnp.transpose(w_qkv, (1, 2, 0)).reshape(3 * cols, width)
    if part_size == 2:
        qkv_other = swap(qkv_own, PART, 2, 1)
        low_part = lax.axis_index(PART) == 0
        qkv_weight = jnp.concatenate(
            [jnp.where(low_part, qkv_own, qkv_other), jnp.where(low_part, qkv_other, qkv_own)]
        )
    else:
        qkv_weight = lax.all_gather(qkv_own, PART, axis=0, tiled=True)
    unit_ids = segment_ids[::unit] - lax.axis_index(DP) * slots
    pick = (unit_ids[:, None] == jnp.arange(slots, dtype=jnp.int32)[None, :]).astype(F32)
    cond_act, silu_back = jax.vjp(jax.nn.silu, cond)
    cond_low = cond_act.astype(BF16)
    cond_all = gather_axis(gather_axis(cond_low, CORE, 2), OUTER, outer_size)
    mod_part = jnp.dot(cond_low, w_ada, preferred_element_type=F32) + b_ada.astype(F32)
    mod_sent = jnp.dot(pick, mod_part, precision=TOP).reshape(head_size, units, ada_cols)
    bias_own = jnp.concatenate([bias_qv[0], jnp.zeros((cols,), bias_qv.dtype), bias_qv[1]])
    mod_sent = jnp.concatenate(
        [
            mod_sent,
            spread_row(b_fc1.astype(F32), head_size, ada_cols),
            spread_row(bias_own.astype(F32), head_size, ada_cols),
        ],
        axis=1,
    )
    mod_got = lax.all_to_all(mod_sent, HEAD, split_axis=0, concat_axis=0, tiled=True)
    bias_fc1 = jnp.transpose(
        mod_got[:, units, :ff_here].reshape(head_size, 2, ff_here // 2), (1, 0, 2)
    ).reshape(-1)
    bias_parts = mod_got[:, units + 1, : 3 * cols].reshape(part_size, group_size, 3 * cols)
    qkv_bias = lax.dynamic_slice_in_dim(
        bias_parts, lax.axis_index(GROUP), 1, axis=1
    ).reshape(part_size * 3 * cols)
    modulation = jnp.transpose(mod_got[:, :units], (1, 0, 2)).reshape(units, 6, 1, width)
    shift_a, scale_a, gate_a, shift_m, scale_m, gate_m = [modulation[:, i] for i in range(6)]

    def by_unit(value):
        return value.reshape(units, unit, width)

    def flat(value):
        return value.reshape(rows, width)

    resid = by_unit(tokens.astype(F32))
    normed_a, inverse_a = layer_norm(resid)
    attn_in = flat((normed_a * (1.0 + scale_a) + shift_a).astype(BF16))
    gathered = gather_group(attn_in, group_size)
    qkv = (lax.dot_general(gathered, qkv_weight, NT, preferred_element_type=F32) + qkv_bias).astype(
        BF16
    )
    blocks = gathered.shape[0] // LONG_SEQ
    first = lax.axis_index(PART) * gathered.shape[0] + jnp.arange(blocks) * LONG_SEQ
    single = (segment_ids[first] == segment_ids[first + SHORT_SEQ]).astype(jnp.int32)
    mix_part = attend(single, qkv, heads, cols)
    mix_got = lax.all_to_all(
        mix_part.reshape(group_size, rows, heads * HEAD_DIM), GROUP, split_axis=0, concat_axis=0
    )
    mix_got = mix_got.reshape(group_size, rows, part_size, 2, proj_half)
    mix = jnp.transpose(mix_got, (1, 3, 2, 0, 4)).reshape(rows, width)
    branch_a = by_unit(
        jnp.dot(mix, proj_full, preferred_element_type=F32) + b_proj.astype(F32)
    )
    mid = resid + gate_a * branch_a
    normed_m, inverse_m = layer_norm(mid)
    mlp_in = flat((normed_m * (1.0 + scale_m) + shift_m).astype(BF16))
    cotan = by_unit(cotangent.astype(F32))
    grad_branch_m = flat((gate_m * cotan).astype(BF16))
    branch_m, grad_mlp_in, grad_fc1, grad_fc2, grad_b1 = mlp(
        mlp_in, grad_branch_m, fc1_full, fc2_full, bias_fc1
    )
    grad_fc2 = scatter_weight(grad_fc2)
    grad_fc1 = scatter_weight(grad_fc1)
    branch_m = by_unit(branch_m) + b_fc2.astype(F32)
    grad_mlp_in = by_unit(grad_mlp_in)
    output = flat((mid + gate_m * branch_m).astype(BF16))
    grad_mid = cotan + norm_back(grad_mlp_in * (1.0 + scale_m), normed_m, inverse_m)
    grad_branch_a = flat((gate_a * grad_mid).astype(BF16))
    bias_sums = jnp.concatenate(
        [
            jnp.sum(grad_branch_a.astype(F32), axis=0),
            jnp.sum(grad_branch_m.astype(F32), axis=0),
            grad_b1.reshape(-1),
        ]
    ).reshape(-1, width)
    for axis, size in ((CORE, 2), (OUTER, outer_size), (GROUP, group_size), (PART, part_size)):
        bias_sums = sum_axis(bias_sums, axis, size)
    grad_b_proj, grad_b_fc2 = bias_sums[0], bias_sums[1]
    grad_b1 = lax.dynamic_slice_in_dim(
        bias_sums[2:].reshape(2, head_size, ff_here // 2), head_at, 1, axis=1
    ).reshape(-1)
    grad_mix = lax.dot_general(grad_branch_a, proj_full, NT, preferred_element_type=F32)
    grad_mix = grad_mix.astype(BF16).reshape(rows, 2, part_size, group_size, proj_half)
    grad_mix = jnp.transpose(grad_mix, (3, 0, 2, 1, 4)).reshape(group_size, rows, -1)
    grad_mix = lax.all_to_all(grad_mix, GROUP, split_axis=0, concat_axis=0)
    grad_proj = lax.dot_general(mix, grad_branch_a, TN, preferred_element_type=F32).astype(BF16)
    grad_proj = scatter_weight(grad_proj)
    grad_qkv = attend_back(single, qkv, grad_mix.reshape(-1, heads * HEAD_DIM), heads, cols)
    attn_grad_part = jnp.dot(grad_qkv, qkv_weight, preferred_element_type=F32).astype(BF16)
    grad_attn_in = by_unit(scatter_group(attn_grad_part, group_size))

    grad_w_qkv = lax.dot_general(grad_qkv, gathered, TN, preferred_element_type=F32)
    grad_bias = jnp.sum(grad_qkv.astype(F32), axis=0)
    bias_rows = jnp.pad(grad_bias.reshape(part_size, 1, 3 * cols), ((0, 0), (0, 0), (0, width - 3 * cols)))
    pad_rows = jnp.zeros((part_size, 15, width), F32)
    grad_w_qkv = jnp.concatenate(
        [grad_w_qkv.reshape(part_size, 3 * cols, width), bias_rows, pad_rows], axis=1
    ).astype(BF16)
    if part_size == 2:
        mine, theirs = grad_w_qkv[0], grad_w_qkv[1]
        low_part = lax.axis_index(PART) == 0
        kept = jnp.where(low_part, mine, theirs)
        sent = jnp.where(low_part, theirs, mine)
        grad_w_qkv = kept.astype(F32) + swap(sent, PART, 2, 1).astype(F32)
    else:
        grad_w_qkv = lax.psum_scatter(
            grad_w_qkv, PART, scatter_dimension=0, tiled=True
        )[0].astype(F32)
    grad_w_qkv = sum_cores(grad_w_qkv).astype(BF16)
    grad_w_qkv = join_cores(sum_outer(grad_w_qkv, outer_size)).astype(F32)
    grad_bias = grad_w_qkv[3 * cols, : 3 * cols]
    grad_bias_qv = jnp.stack([grad_bias[:cols], grad_bias[2 * cols :]])
    grad_w_qkv = jnp.transpose(grad_w_qkv[: 3 * cols].reshape(3, cols, width), (2, 0, 1))

    grad_fc2 = join_cores(sum_outer(grad_fc2, outer_size)).astype(F32)
    grad_fc1 = join_cores(sum_outer(grad_fc1, outer_size)).astype(F32).T
    grad_proj = join_cores(sum_outer(grad_proj, outer_size)).astype(F32)

    grad_tokens = flat(
        (grad_mid + norm_back(grad_attn_in * (1.0 + scale_a), normed_a, inverse_a)).astype(BF16)
    )
    unit_grad = jnp.concatenate(
        [
            jnp.sum(value, axis=1)
            for value in (
                grad_attn_in,
                grad_attn_in * normed_a,
                grad_mid * branch_a,
                grad_mlp_in,
                grad_mlp_in * normed_m,
                cotan * branch_m,
            )
        ],
        axis=1,
    )
    unit_grad = jnp.transpose(unit_grad.reshape(units, head_size, ada_cols), (1, 0, 2))
    unit_grad = lax.all_to_all(unit_grad, HEAD, split_axis=0, concat_axis=0, tiled=True)
    grad_mod = lax.dot_general(
        pick, unit_grad.reshape(head_size * units, ada_cols), TN, precision=TOP
    )
    grad_mod_all = gather_axis(gather_axis(grad_mod, CORE, 2), OUTER, outer_size)
    grad_w_ada = lax.dot_general(cond_all.astype(F32), grad_mod_all, TN, precision=TOP)
    grad_b_ada = jnp.sum(grad_mod_all, axis=0)
    grad_cond_part = lax.dot_general(grad_mod, w_ada.astype(F32), NT, precision=TOP)
    grad_cond_sum = sum_axis(sum_axis(grad_cond_part, GROUP, group_size), PART, part_size)
    grad_cond = silu_back(grad_cond_sum)[0]
    return (
        output,
        grad_tokens,
        grad_cond,
        grad_w_ada,
        grad_b_ada,
        grad_w_qkv,
        grad_bias_qv,
        grad_proj,
        grad_b_proj,
        grad_fc1,
        grad_b1,
        grad_fc2,
        grad_b_fc2,
    )


def solution(mesh):
    dp_size, head_size = mesh.shape["dp"], mesh.shape["head"]

    def run(*arrays):
        rows = arrays[0].shape[0] // (dp_size * head_size)
        group_size = math.lcm(rows, LONG_SEQ) // rows
        sizes = (dp_size // 2, head_size // group_size, group_size)
        finer = Mesh(
            mesh.devices.reshape(sizes[0], 2, sizes[1], sizes[2]), (OUTER, CORE, PART, GROUP)
        )
        placed = (
            P(EVERY, None),
            P(DP),
            P(DP, None),
            P(None, HEAD),
            P(HEAD),
            P(None, None, HEAD),
            P(None, HEAD),
            P(HEAD, None),
            P(),
            P(None, HEAD),
            P(HEAD),
            P(HEAD, None),
            P(),
            P(EVERY, None),
        )
        results = (
            P(EVERY, None),
            P(EVERY, None),
            P(DP, None),
            P(None, HEAD),
            P(HEAD),
            P(None, None, HEAD),
            P(None, HEAD),
            P(HEAD, None),
            P(),
            P(None, HEAD),
            P(HEAD),
            P(HEAD, None),
            P(),
        )
        return jax.shard_map(
            functools.partial(local, sizes),
            mesh=finer,
            in_specs=placed,
            out_specs=results,
            check_vma=False,
        )(*arrays)

    return run
```

```python
import functools
import math

import jax
import jax.numpy as jnp
from jax import lax
from jax.experimental import pallas as pl
from jax.experimental.pallas import tpu as pltpu
from jax.sharding import Mesh
from jax.sharding import PartitionSpec as P

HEAD_DIM = 72
LONG_SEQ = 1024
SHORT_SEQ = 256
LANES = 128
NORM_EPS = 1e-06
TOP = lax.Precision.HIGHEST
F32 = jnp.float32
BF16 = jnp.bfloat16

OUTER, CORE, PART, GROUP = "outer", "core", "part", "group"
DP = (OUTER, CORE)
HEAD = (PART, GROUP)
SPREAD = (CORE, PART, GROUP)
EVERY = (OUTER, CORE, PART, GROUP)

NT = (((1,), (1,)), ((), ()))
TN = (((0,), (0,)), ((), ()))


def layer_norm(values):
    centered = values - jnp.mean(values, axis=-1, keepdims=True)
    inverse = lax.rsqrt(jnp.mean(centered * centered, axis=-1, keepdims=True) + NORM_EPS)
    return (centered * inverse, inverse)


def norm_back(grad_normed, normed, inverse):
    mean_grad = jnp.mean(grad_normed, axis=-1, keepdims=True)
    mean_cross = jnp.mean(grad_normed * normed, axis=-1, keepdims=True)
    return inverse * (grad_normed - mean_grad - normed * mean_cross)


def head_columns(index, cols, offset):
    per_shard = cols // HEAD_DIM
    shard, within = index // per_shard, index % per_shard
    return shard * 3 * cols + offset * cols + within * HEAD_DIM


def attend_kernel(heads, cols, single_ref, qkv_ref, mix_ref, q_s, k_s, v_s, o_s):
    scale = 1.0 / math.sqrt(HEAD_DIM)
    units = LONG_SEQ // SHORT_SEQ
    pad = jnp.zeros((LONG_SEQ, LANES - HEAD_DIM), BF16)
    for h in range(heads):
        for offset, ref in enumerate((q_s, k_s, v_s)):
            at = head_columns(h, cols, offset)
            ref[h, :, :HEAD_DIM] = qkv_ref[:, at : at + HEAD_DIM]
            ref[h, :, HEAD_DIM:] = pad

    def attend_keys(h, rows, key_rows):
        scores = (
            lax.dot_general(q_s[h, rows], k_s[h, key_rows], NT, preferred_element_type=F32) * scale
        )
        weights = jnp.exp(scores - jnp.max(scores, axis=-1, keepdims=True))
        probs = weights * (1.0 / jnp.sum(weights, axis=-1, keepdims=True))
        o_s[h, rows] = jnp.dot(
            probs.astype(BF16), v_s[h, key_rows], preferred_element_type=F32
        ).astype(BF16)

    def step(i, carry):
        h = i // units
        rows = pl.ds(pl.multiple_of((i % units) * SHORT_SEQ, SHORT_SEQ), SHORT_SEQ)

        @pl.when(single_ref[pl.program_id(0)] == 1)
        def _():
            attend_keys(h, rows, slice(None))

        @pl.when(single_ref[pl.program_id(0)] == 0)
        def _():
            attend_keys(h, rows, rows)

        return carry

    lax.fori_loop(0, heads * units, step, 0)
    for h in range(heads):
        mix_ref[:, h * HEAD_DIM : (h + 1) * HEAD_DIM] = o_s[h, :, :HEAD_DIM]


def attend(single, qkv, heads, cols):
    rows, width = qkv.shape
    blocks = rows // LONG_SEQ
    return pl.pallas_call(
        functools.partial(attend_kernel, heads, cols),
        grid_spec=pltpu.PrefetchScalarGridSpec(
            num_scalar_prefetch=1,
            grid=(blocks,),
            in_specs=[pl.BlockSpec((LONG_SEQ, width), lambda b, s: (b, 0))],
            out_specs=pl.BlockSpec((LONG_SEQ, heads * HEAD_DIM), lambda b, s: (b, 0)),
            scratch_shapes=[pltpu.VMEM((heads, LONG_SEQ, LANES), BF16)] * 4,
        ),
        out_shape=jax.ShapeDtypeStruct((rows, heads * HEAD_DIM), BF16),
        cost_estimate=pl.CostEstimate(
            flops=4 * rows * LONG_SEQ * heads * LANES,
            bytes_accessed=2 * rows * (width + heads * HEAD_DIM),
            transcendentals=rows * LONG_SEQ * heads,
        ),
        name="attend",
    )(single, qkv)


def attend_back_kernel(
    heads, cols, single_ref, qkv_ref, grad_ref, out_ref, q_s, k_s, v_s, g_s, dq_s, dk_s, dv_s, kt_s
):
    scale = 1.0 / math.sqrt(HEAD_DIM)
    units = LONG_SEQ // SHORT_SEQ
    pad = jnp.zeros((LONG_SEQ, LANES - HEAD_DIM), BF16)
    for h in range(heads):
        for offset, ref in enumerate((q_s, k_s, v_s)):
            at = head_columns(h, cols, offset)
            ref[h, :, :HEAD_DIM] = qkv_ref[:, at : at + HEAD_DIM]
            ref[h, :, HEAD_DIM:] = pad
        g_s[h, :, :HEAD_DIM] = grad_ref[:, h * HEAD_DIM : (h + 1) * HEAD_DIM]
        g_s[h, :, HEAD_DIM:] = pad
        kt_s[h] = k_s[h].T
    is_single = single_ref[pl.program_id(0)] == 1

    def grads(h, rows, key_rows):
        q, g = q_s[h, rows], g_s[h, rows]
        k, v = k_s[h, key_rows], v_s[h, key_rows]
        scores = lax.dot_general(k, q, NT, preferred_element_type=F32) * scale
        weights = jnp.exp(scores - jnp.max(scores, axis=0, keepdims=True))
        probs = weights * (1.0 / jnp.sum(weights, axis=0, keepdims=True))
        grad_probs = lax.dot_general(v, g, NT, preferred_element_type=F32)
        inner = jnp.sum(probs * grad_probs, axis=0, keepdims=True)
        grad_scores = (probs * (grad_probs - inner)).astype(BF16)
        grad_v = jnp.dot(probs.astype(BF16), g, preferred_element_type=F32)
        grad_k = jnp.dot(grad_scores, q, preferred_element_type=F32)
        grad_q = jnp.dot(kt_s[h, :, key_rows], grad_scores, preferred_element_type=F32)
        dq_s[h, rows] = (grad_q.T * scale).astype(BF16)
        return grad_k, grad_v

    @pl.when(is_single)
    def _():
        dk_s[...] = jnp.zeros_like(dk_s)
        dv_s[...] = jnp.zeros_like(dv_s)

    def step(i, carry):
        h = i // units
        rows = pl.ds(pl.multiple_of((i % units) * SHORT_SEQ, SHORT_SEQ), SHORT_SEQ)

        @pl.when(is_single)
        def _():
            grad_k, grad_v = grads(h, rows, slice(None))
            dk_s[h] += grad_k
            dv_s[h] += grad_v

        @pl.when(jnp.logical_not(is_single))
        def _():
            grad_k, grad_v = grads(h, rows, rows)
            dk_s[h, rows] = grad_k
            dv_s[h, rows] = grad_v

        return carry

    lax.fori_loop(0, heads * units, step, 0)
    for h in range(heads):
        for offset, value in enumerate(
            (dq_s[h], (dk_s[h] * scale).astype(BF16), dv_s[h].astype(BF16))
        ):
            at = head_columns(h, cols, offset)
            out_ref[:, at : at + HEAD_DIM] = value[:, :HEAD_DIM]


def attend_back(single, qkv, grad_mix, heads, cols):
    rows, width = qkv.shape
    blocks = rows // LONG_SEQ
    low = pltpu.VMEM((heads, LONG_SEQ, LANES), BF16)
    wide = pltpu.VMEM((heads, LONG_SEQ, LANES), F32)
    return pl.pallas_call(
        functools.partial(attend_back_kernel, heads, cols),
        grid_spec=pltpu.PrefetchScalarGridSpec(
            num_scalar_prefetch=1,
            grid=(blocks,),
            in_specs=[
                pl.BlockSpec((LONG_SEQ, width), lambda b, s: (b, 0)),
                pl.BlockSpec((LONG_SEQ, heads * HEAD_DIM), lambda b, s: (b, 0)),
            ],
            out_specs=pl.BlockSpec((LONG_SEQ, width), lambda b, s: (b, 0)),
            scratch_shapes=[low] * 5 + [wide] * 2 + [pltpu.VMEM((heads, LANES, LONG_SEQ), BF16)],
        ),
        out_shape=jax.ShapeDtypeStruct((rows, width), BF16),
        cost_estimate=pl.CostEstimate(
            flops=10 * rows * LONG_SEQ * heads * LANES,
            bytes_accessed=2 * rows * (2 * width + heads * HEAD_DIM),
            transcendentals=rows * LONG_SEQ * heads,
        ),
        name="attend_back",
    )(single, qkv, grad_mix)


def mlp_kernel(
    x_ref, xo_ref, g_ref, go_ref, w1_ref, w2_ref, b1_ref,
    out_ref, outo_ref, gin_ref, gino_ref, d1_ref, d2_ref, db_ref,
    x_s, g_s, acc_s, gacc_s,
):
    rows = x_ref.shape[0]

    @pl.when(pl.program_id(0) == 0)
    def _():
        x_s[:rows], x_s[rows:] = x_ref[...], xo_ref[...]
        g_s[:rows], g_s[rows:] = g_ref[...], go_ref[...]
        for ref in (out_ref, gin_ref, acc_s, gacc_s):
            ref[...] = jnp.zeros_like(ref)

    root = math.sqrt(2.0 / math.pi)
    w1, w2 = w1_ref[...], w2_ref[...]
    pre = lax.dot_general(x_s[...], w1, NT, preferred_element_type=F32) + b1_ref[0]
    grad_hidden = lax.dot_general(g_s[...], w2, NT, preferred_element_type=F32)
    square = pre * pre
    bent = jnp.tanh(root * (pre * (1.0 + 0.044715 * square)))
    half = 0.5 * (1.0 + bent)
    slope = half + (0.5 * root) * pre * (1.0 - bent * bent) * (1.0 + (3 * 0.044715) * square)
    hidden = (pre * half).astype(BF16)
    grad_pre = (grad_hidden * slope).astype(BF16)
    out_ref[...] += jnp.dot(hidden[:rows], w2, preferred_element_type=F32)
    acc_s[...] += jnp.dot(hidden[rows:], w2, preferred_element_type=F32)
    gin_ref[...] += jnp.dot(grad_pre[:rows], w1, preferred_element_type=F32)
    gacc_s[...] += jnp.dot(grad_pre[rows:], w1, preferred_element_type=F32)
    d2_ref[...] = lax.dot_general(hidden, g_s[...], TN, preferred_element_type=F32).astype(BF16)
    d1_ref[...] = lax.dot_general(grad_pre, x_s[...], TN, preferred_element_type=F32).astype(BF16)
    db_ref[0] = jnp.sum(grad_pre.astype(F32), axis=0, keepdims=True)

    @pl.when(pl.program_id(0) == pl.num_programs(0) - 1)
    def _():
        outo_ref[...] = acc_s[...].astype(BF16)
        gino_ref[...] = gacc_s[...].astype(BF16)


def mlp(x, x_other, g, g_other, w1, w2, b1):
    rows, width = x.shape
    units = w1.shape[0]
    tile = next(t for t in (256, 128) if units % t == 0)
    tiles = units // tile
    given = pl.BlockSpec((rows, width), lambda f: (0, 0), pipeline_mode=pl.Buffered(1))
    whole = pl.BlockSpec((rows, width), lambda f: (0, 0))
    piece = pl.BlockSpec((tile, width), lambda f: (f, 0))
    line = pl.BlockSpec((1, 1, tile), lambda f: (f, 0, 0))
    return pl.pallas_call(
        mlp_kernel,
        grid=(tiles,),
        in_specs=[given] * 4 + [piece, piece, line],
        out_specs=[whole] * 4 + [piece, piece, line],
        out_shape=[
            jax.ShapeDtypeStruct((rows, width), F32),
            jax.ShapeDtypeStruct((rows, width), BF16),
            jax.ShapeDtypeStruct((rows, width), F32),
            jax.ShapeDtypeStruct((rows, width), BF16),
            jax.ShapeDtypeStruct((units, width), BF16),
            jax.ShapeDtypeStruct((units, width), BF16),
            jax.ShapeDtypeStruct((tiles, 1, tile), F32),
        ],
        scratch_shapes=[pltpu.VMEM((2 * rows, width), BF16)] * 2
        + [pltpu.VMEM((rows, width), F32)] * 2,
        cost_estimate=pl.CostEstimate(
            flops=24 * rows * width * units,
            bytes_accessed=8 * units * width + 20 * rows * width,
            transcendentals=2 * rows * units,
        ),
        name="mlp",
    )(x, x_other, g, g_other, w1, w2, b1.reshape(tiles, 1, tile))


def xor_pairs(size, mask):
    return [(i, i ^ mask) for i in range(size)]


def swap(value, axis, size, mask):
    return lax.ppermute(value, axis, xor_pairs(size, mask))


def gather_group(own, size):
    rows = own.shape[0]
    me = lax.axis_index(GROUP)
    if size != 4:
        return lax.all_gather(own, GROUP, axis=0, tiled=True)
    half = rows // 2
    near = swap(own, GROUP, 4, 1)
    far = swap(own, GROUP, 4, 2)
    upper = swap(far[:half], GROUP, 4, 1)
    lower = swap(near[half:], GROUP, 4, 2)
    whole = jnp.zeros((4 * rows, own.shape[1]), own.dtype)
    for mask, at, piece in (
        (0, 0, own),
        (1, 0, near),
        (2, 0, far),
        (3, 0, upper),
        (3, half, lower),
    ):
        start = jnp.bitwise_xor(me, mask) * rows + at
        whole = lax.dynamic_update_slice_in_dim(whole, piece, start, 0)
    return whole


def scatter_group(partial, size):
    if size != 4:
        return lax.psum_scatter(partial, GROUP, scatter_dimension=0, tiled=True).astype(F32)
    rows = partial.shape[0] // 4
    half = rows // 2
    me = lax.axis_index(GROUP)

    def piece(mask, at):
        start = jnp.bitwise_xor(me, mask) * rows + at
        return lax.dynamic_slice_in_dim(partial, start, half)

    upper = swap(jnp.stack([piece(1, 0), piece(3, 0)]), GROUP, 4, 1)
    lower = swap(jnp.stack([piece(2, half), piece(3, half)]), GROUP, 4, 2)
    upper_far = swap((piece(2, 0).astype(F32) + upper[1].astype(F32)).astype(BF16), GROUP, 4, 2)
    lower_far = swap((piece(1, half).astype(F32) + lower[1].astype(F32)).astype(BF16), GROUP, 4, 1)
    return jnp.concatenate(
        [
            piece(0, 0).astype(F32) + upper[0].astype(F32) + upper_far.astype(F32),
            piece(0, half).astype(F32) + lower[0].astype(F32) + lower_far.astype(F32),
        ]
    )


def powers(size):
    return [1 << b for b in range(size.bit_length() - 1)] if size & (size - 1) == 0 else None


def sum_axis(value, axis, size):
    masks = powers(size)
    if masks is None:
        return lax.psum(value, axis)
    for mask in masks:
        value = value + swap(value, axis, size, mask)
    return value


def gather_axis(value, axis, size):
    masks = powers(size)
    if masks is None:
        return lax.all_gather(value, axis, axis=0, tiled=True)
    me = lax.axis_index(axis)
    for mask in masks:
        other = swap(value, axis, size, mask)
        first = jnp.bitwise_and(me, mask) == 0
        value = jnp.concatenate(
            [jnp.where(first, value, other), jnp.where(first, other, value)], axis=0
        )
    return value


def sum_outer(value, size):
    total = value.astype(F32)
    masks = powers(size)
    if masks is None:
        return lax.psum(value, OUTER).astype(F32)
    for mask in masks:
        low = total.astype(BF16)
        total = low.astype(F32) + swap(low, OUTER, size, mask).astype(F32)
    return total


def sum_cores(value):
    half = value.shape[0] // 2
    sent = lax.dynamic_slice_in_dim(value, (1 - lax.axis_index(CORE)) * half, half)
    got = swap(sent.astype(BF16), CORE, 2, 1)
    return core_half(value).astype(F32) + got.astype(F32)


def join_cores(own):
    own = own.astype(BF16)
    other = swap(own, CORE, 2, 1)
    first = lax.axis_index(CORE) == 0
    return jnp.concatenate([jnp.where(first, own, other), jnp.where(first, other, own)])


def gather_weight(shard, planes):
    if planes != 2:
        return core_half(lax.all_gather(core_half(shard), SPREAD, axis=0, tiled=True))
    quarter = shard.shape[0] // 4
    at = (lax.axis_index(OUTER) * 2 + lax.axis_index(CORE)) * quarter
    return core_half(
        lax.all_gather(lax.dynamic_slice_in_dim(shard, at, quarter), SPREAD, axis=0, tiled=True)
    )


def cross_planes(mine, planes):
    return jnp.concatenate([mine, swap(mine, OUTER, 2, 1)]) if planes == 2 else mine


def order_units(rows, planes):
    heads, units = rows.shape
    core = lax.axis_index(CORE)
    if planes != 2:
        halves = jnp.transpose(rows.reshape(heads, 2, units // 2), (1, 0, 2))
        return jnp.where(core == 0, halves[0], halves[1]).reshape(-1)
    quarters = jnp.transpose(rows.reshape(heads, 2, 2, units // 4), (2, 1, 0, 3))
    quarters = jnp.where(core == 0, quarters[0], quarters[1])
    return jnp.where(lax.axis_index(OUTER) == 0, quarters, quarters[::-1]).reshape(-1)


def restore_units(mine, heads, planes):
    core = lax.axis_index(CORE)
    if planes != 2:
        mine = mine.reshape(heads, 1, -1)
    else:
        mine = mine.reshape(2, heads, -1)
        mine = jnp.where(lax.axis_index(OUTER) == 0, mine, mine[::-1])
        mine = jnp.transpose(mine, (1, 0, 2))
    none = jnp.zeros_like(mine)
    both = jnp.stack([jnp.where(core == 0, mine, none), jnp.where(core == 0, none, mine)], axis=2)
    return both.reshape(heads, -1)


def join_planes(quarter):
    across = swap(quarter, OUTER, 2, 1)
    first = lax.axis_index(OUTER) == 0
    pair = jnp.stack([jnp.where(first, across, quarter), jnp.where(first, quarter, across)])
    beside = swap(pair, CORE, 2, 1)
    first = lax.axis_index(CORE) == 0
    whole = jnp.stack([jnp.where(first, pair, beside), jnp.where(first, beside, pair)], axis=1)
    return whole.reshape(-1, quarter.shape[1]).astype(F32)


def scatter_weight(value):
    value = sum_cores(value).astype(BF16)
    return lax.psum_scatter(value, HEAD, scatter_dimension=0, tiled=True)


def core_half(value):
    half = value.shape[0] // 2
    return lax.dynamic_slice_in_dim(value, lax.axis_index(CORE) * half, half)


def spread_row(row, copies, width):
    row = jnp.pad(row, (0, width - row.shape[0]))
    return jnp.broadcast_to(row, (copies, 1, width))


def local(
    sizes,
    tokens,
    segment_ids,
    cond,
    w_ada,
    b_ada,
    w_qkv,
    bias_qv,
    w_proj,
    b_proj,
    w_fc1,
    b_fc1,
    w_fc2,
    b_fc2,
    cotangent,
):
    outer_size, part_size, group_size = sizes
    head_size = part_size * group_size
    rows, width = tokens.shape
    slots = cond.shape[0]
    cols = w_qkv.shape[2]
    ada_cols = w_ada.shape[1]
    ff_here = w_fc1.shape[1]
    unit = math.gcd(rows, SHORT_SEQ)
    units = rows // unit
    heads = part_size * cols // HEAD_DIM
    head_at = lax.axis_index(HEAD)

    fc1_mine = gather_weight(w_fc1.T, outer_size)
    fc2_mine = gather_weight(w_fc2, outer_size)
    proj_half = cols // 2
    proj_full = lax.all_gather(core_half(w_proj), SPREAD, axis=0, tiled=True)
    qkv_own = jnp.transpose(w_qkv, (1, 2, 0)).reshape(3 * cols, width)
    if part_size == 2:
        qkv_other = swap(qkv_own, PART, 2, 1)
        low_part = lax.axis_index(PART) == 0
        qkv_weight = jnp.concatenate(
            [jnp.where(low_part, qkv_own, qkv_other), jnp.where(low_part, qkv_other, qkv_own)]
        )
    else:
        qkv_weight = lax.all_gather(qkv_own, PART, axis=0, tiled=True)
    unit_ids = segment_ids[::unit] - lax.axis_index(DP) * slots
    pick = (unit_ids[:, None] == jnp.arange(slots, dtype=jnp.int32)[None, :]).astype(F32)
    cond_act, silu_back = jax.vjp(jax.nn.silu, cond)
    cond_low = cond_act.astype(BF16)
    cond_all = gather_axis(gather_axis(cond_low, CORE, 2), OUTER, outer_size)
    mod_part = jnp.dot(cond_low, w_ada, preferred_element_type=F32) + b_ada.astype(F32)
    mod_sent = jnp.dot(pick, mod_part, precision=TOP).reshape(head_size, units, ada_cols)
    bias_own = jnp.concatenate([bias_qv[0], jnp.zeros((cols,), bias_qv.dtype), bias_qv[1]])
    mod_sent = jnp.concatenate(
        [
            mod_sent,
            spread_row(b_fc1.astype(F32), head_size, ada_cols),
            spread_row(bias_own.astype(F32), head_size, ada_cols),
        ],
        axis=1,
    )
    mod_got = lax.all_to_all(mod_sent, HEAD, split_axis=0, concat_axis=0, tiled=True)
    bias_fc1 = order_units(mod_got[:, units, :ff_here], outer_size)
    bias_parts = mod_got[:, units + 1, : 3 * cols].reshape(part_size, group_size, 3 * cols)
    qkv_bias = lax.dynamic_slice_in_dim(
        bias_parts, lax.axis_index(GROUP), 1, axis=1
    ).reshape(part_size * 3 * cols)
    modulation = jnp.transpose(mod_got[:, :units], (1, 0, 2)).reshape(units, 6, 1, width)
    shift_a, scale_a, gate_a, shift_m, scale_m, gate_m = [modulation[:, i] for i in range(6)]

    def by_unit(value):
        return value.reshape(units, unit, width)

    def flat(value):
        return value.reshape(rows, width)

    resid = by_unit(tokens.astype(F32))
    normed_a, inverse_a = layer_norm(resid)
    attn_in = flat((normed_a * (1.0 + scale_a) + shift_a).astype(BF16))
    gathered = gather_group(attn_in, group_size)
    gathered, fc1_mine, fc2_mine = lax.optimization_barrier((gathered, fc1_mine, fc2_mine))
    fc1_here = cross_planes(fc1_mine, outer_size)
    fc2_here = cross_planes(fc2_mine, outer_size)
    qkv = (lax.dot_general(gathered, qkv_weight, NT, preferred_element_type=F32) + qkv_bias).astype(
        BF16
    )
    blocks = gathered.shape[0] // LONG_SEQ
    first = lax.axis_index(PART) * gathered.shape[0] + jnp.arange(blocks) * LONG_SEQ
    single = (segment_ids[first] == segment_ids[first + SHORT_SEQ]).astype(jnp.int32)
    mix_part = attend(single, qkv, heads, cols)
    mix_got = lax.all_to_all(
        mix_part.reshape(group_size, rows, heads * HEAD_DIM), GROUP, split_axis=0, concat_axis=0
    )
    mix_got = mix_got.reshape(group_size, rows, part_size, 2, proj_half)
    mix = jnp.transpose(mix_got, (1, 3, 2, 0, 4)).reshape(rows, width)
    branch_a = by_unit(
        jnp.dot(mix, proj_full, preferred_element_type=F32) + b_proj.astype(F32)
    )
    mid = resid + gate_a * branch_a
    normed_m, inverse_m = layer_norm(mid)
    mlp_in = flat((normed_m * (1.0 + scale_m) + shift_m).astype(BF16))
    cotan = by_unit(cotangent.astype(F32))
    grad_branch_m = flat((gate_m * cotan).astype(BF16))
    branch_m, branch_beside, grad_mlp_in, grad_beside, grad_fc1, grad_fc2, grad_b1 = mlp(
        mlp_in,
        swap(mlp_in, CORE, 2, 1),
        grad_branch_m,
        swap(grad_branch_m, CORE, 2, 1),
        fc1_here,
        fc2_here,
        bias_fc1,
    )
    grad_mlp_in = by_unit(grad_mlp_in + swap(grad_beside, CORE, 2, 1).astype(F32))
    branch_m = by_unit(
        branch_m + swap(branch_beside, CORE, 2, 1).astype(F32) + b_fc2.astype(F32)
    )
    if outer_size == 2:
        half = grad_fc2.shape[0] // 2
        crossed_fc2 = swap(grad_fc2[:half], OUTER, 2, 1)
        sent_fc1, crossed_fc2 = lax.optimization_barrier((grad_fc1[:half], crossed_fc2))
        crossed_fc1 = swap(sent_fc1, OUTER, 2, 1)
        grad_fc2 = (grad_fc2[half:].astype(F32) + crossed_fc2.astype(F32)).astype(BF16)
        grad_fc1 = (grad_fc1[half:].astype(F32) + crossed_fc1.astype(F32)).astype(BF16)
    grad_b1 = restore_units(grad_b1.reshape(-1), head_size, outer_size)
    output = flat((mid + gate_m * branch_m).astype(BF16))
    grad_mid = cotan + norm_back(grad_mlp_in * (1.0 + scale_m), normed_m, inverse_m)
    grad_branch_a = flat((gate_a * grad_mid).astype(BF16))
    bias_sums = jnp.concatenate(
        [
            jnp.sum(grad_branch_a.astype(F32), axis=0),
            jnp.sum(grad_branch_m.astype(F32), axis=0),
            grad_b1.reshape(-1),
        ]
    ).reshape(-1, width)
    for axis, size in ((CORE, 2), (OUTER, outer_size), (GROUP, group_size), (PART, part_size)):
        bias_sums = sum_axis(bias_sums, axis, size)
    grad_b_proj, grad_b_fc2 = bias_sums[0], bias_sums[1]
    grad_b1 = lax.dynamic_slice_in_dim(
        bias_sums[2:].reshape(head_size, ff_here), head_at, 1
    ).reshape(-1)
    grad_mix = lax.dot_general(grad_branch_a, proj_full, NT, preferred_element_type=F32)
    grad_mix = grad_mix.astype(BF16).reshape(rows, 2, part_size, group_size, proj_half)
    grad_mix = jnp.transpose(grad_mix, (3, 0, 2, 1, 4)).reshape(group_size, rows, -1)
    grad_mix = lax.all_to_all(grad_mix, GROUP, split_axis=0, concat_axis=0)
    grad_mix, grad_fc2 = lax.optimization_barrier((grad_mix, grad_fc2))
    grad_proj = lax.dot_general(mix, grad_branch_a, TN, preferred_element_type=F32).astype(BF16)
    grad_proj = scatter_weight(grad_proj)
    scattered_fc2 = lax.psum_scatter(grad_fc2, HEAD, scatter_dimension=0, tiled=True)
    scattered_fc1 = lax.psum_scatter(grad_fc1, HEAD, scatter_dimension=0, tiled=True)
    grad_qkv = attend_back(single, qkv, grad_mix.reshape(-1, heads * HEAD_DIM), heads, cols)
    attn_grad_part = jnp.dot(grad_qkv, qkv_weight, preferred_element_type=F32).astype(BF16)
    attn_grad_part, grad_qkv = lax.optimization_barrier((attn_grad_part, grad_qkv))
    grad_attn_in = by_unit(scatter_group(attn_grad_part, group_size))

    grad_w_qkv = lax.dot_general(grad_qkv, gathered, TN, preferred_element_type=F32)
    grad_bias = jnp.sum(grad_qkv.astype(F32), axis=0)
    bias_rows = jnp.pad(grad_bias.reshape(part_size, 1, 3 * cols), ((0, 0), (0, 0), (0, width - 3 * cols)))
    pad_rows = jnp.zeros((part_size, 15, width), F32)
    grad_w_qkv = jnp.concatenate(
        [grad_w_qkv.reshape(part_size, 3 * cols, width), bias_rows, pad_rows], axis=1
    ).astype(BF16)
    if part_size == 2:
        mine, theirs = grad_w_qkv[0], grad_w_qkv[1]
        low_part = lax.axis_index(PART) == 0
        kept = jnp.where(low_part, mine, theirs)
        sent = jnp.where(low_part, theirs, mine)
        grad_w_qkv = kept.astype(F32) + swap(sent, PART, 2, 1).astype(F32)
    else:
        grad_w_qkv = lax.psum_scatter(
            grad_w_qkv, PART, scatter_dimension=0, tiled=True
        )[0].astype(F32)
    grad_w_qkv = sum_cores(grad_w_qkv).astype(BF16)
    grad_w_qkv = join_cores(sum_outer(grad_w_qkv, outer_size)).astype(F32)
    grad_bias = grad_w_qkv[3 * cols, : 3 * cols]
    grad_bias_qv = jnp.stack([grad_bias[:cols], grad_bias[2 * cols :]])
    grad_w_qkv = jnp.transpose(grad_w_qkv[: 3 * cols].reshape(3, cols, width), (2, 0, 1))

    if outer_size == 2:
        grad_fc2 = join_planes(scattered_fc2)
        grad_fc1 = join_planes(scattered_fc1).T
    else:
        grad_fc2 = join_cores(sum_outer(scattered_fc2, outer_size)).astype(F32)
        grad_fc1 = join_cores(sum_outer(scattered_fc1, outer_size)).astype(F32).T
    grad_proj = join_cores(sum_outer(grad_proj, outer_size)).astype(F32)

    grad_tokens = flat(
        (grad_mid + norm_back(grad_attn_in * (1.0 + scale_a), normed_a, inverse_a)).astype(BF16)
    )
    unit_grad = jnp.concatenate(
        [
            jnp.sum(value, axis=1)
            for value in (
                grad_attn_in,
                grad_attn_in * normed_a,
                grad_mid * branch_a,
                grad_mlp_in,
                grad_mlp_in * normed_m,
                cotan * branch_m,
            )
        ],
        axis=1,
    )
    unit_grad = jnp.transpose(unit_grad.reshape(units, head_size, ada_cols), (1, 0, 2))
    unit_grad = lax.all_to_all(unit_grad, HEAD, split_axis=0, concat_axis=0, tiled=True)
    grad_mod = lax.dot_general(
        pick, unit_grad.reshape(head_size * units, ada_cols), TN, precision=TOP
    )
    grad_mod_all = gather_axis(gather_axis(grad_mod, CORE, 2), OUTER, outer_size)
    grad_w_ada = lax.dot_general(cond_all.astype(F32), grad_mod_all, TN, precision=TOP)
    grad_b_ada = jnp.sum(grad_mod_all, axis=0)
    grad_cond_part = lax.dot_general(grad_mod, w_ada.astype(F32), NT, precision=TOP)
    grad_cond_sum = sum_axis(sum_axis(grad_cond_part, GROUP, group_size), PART, part_size)
    grad_cond = silu_back(grad_cond_sum)[0]
    return (
        output,
        grad_tokens,
        grad_cond,
        grad_w_ada,
        grad_b_ada,
        grad_w_qkv,
        grad_bias_qv,
        grad_proj,
        grad_b_proj,
        grad_fc1,
        grad_b1,
        grad_fc2,
        grad_b_fc2,
    )


def solution(mesh):
    dp_size, head_size = mesh.shape["dp"], mesh.shape["head"]

    def run(*arrays):
        rows = arrays[0].shape[0] // (dp_size * head_size)
        group_size = math.lcm(rows, LONG_SEQ) // rows
        sizes = (dp_size // 2, head_size // group_size, group_size)
        finer = Mesh(
            mesh.devices.reshape(sizes[0], 2, sizes[1], sizes[2]), (OUTER, CORE, PART, GROUP)
        )
        placed = (
            P(EVERY, None),
            P(DP),
            P(DP, None),
            P(None, HEAD),
            P(HEAD),
            P(None, None, HEAD),
            P(None, HEAD),
            P(HEAD, None),
            P(),
            P(None, HEAD),
            P(HEAD),
            P(HEAD, None),
            P(),
            P(EVERY, None),
        )
        results = (
            P(EVERY, None),
            P(EVERY, None),
            P(DP, None),
            P(None, HEAD),
            P(HEAD),
            P(None, None, HEAD),
            P(None, HEAD),
            P(HEAD, None),
            P(),
            P(None, HEAD),
            P(HEAD),
            P(HEAD, None),
            P(),
        )
        return jax.shard_map(
            functools.partial(local, sizes),
            mesh=finer,
            in_specs=placed,
            out_specs=results,
            check_vma=False,
        )(*arrays)

    return run
```
